32 devices in a mesh: clips: 2 (over x), seq: 16 (over z, y, core).
Axes of the slice: x: 2, y: 2, z: 4, core: 2. Of those that a mesh axis runs over, the one named last changes fastest.
Arguments:
- video_q: bfloat16 [4096, 1536], P(('clips', 'seq')), parts along dimension 0, may hold values from -200 to 200
- video_k: bfloat16 [4096, 1536], P(('clips', 'seq')), parts along dimension 0, may hold values from -7 to 7
- video_v: bfloat16 [4096, 1536], P(('clips', 'seq')), parts along dimension 0, may hold values from -6 to 6
- audio_q: bfloat16 [256, 1536], P(('clips', 'seq')), parts along dimension 0, may hold values from -200 to 200
- audio_k: bfloat16 [256, 1536], P(('clips', 'seq')), parts along dimension 0, may hold values from -6 to 6
- audio_v: bfloat16 [256, 1536], P(('clips', 'seq')), parts along dimension 0, may hold values from -6 to 6
- radius: int32 [32], P(('clips', 'seq')), parts along dimension 0, may hold values from 1 to 2
- tile_list: int32 [32, 5], P('clips'), parts along dimension 0, may hold values from -1 to 15, as said below
- tile_count: int32 [32], P('clips'), parts along dimension 0, may hold values from 1 to 5, as said below
- video_gain: float32 [1536], replicated, may hold values from 0.5 to 1.5
- audio_gain: float32 [1536], replicated, may hold values from 0.5 to 1.5
Outputs:
- video_out: bfloat16 [4096, 1536], P(('clips', 'seq')), parts along dimension 0
- audio_out: bfloat16 [256, 1536], P(('clips', 'seq')), parts along dimension 0
The draws below stay inside these ranges and needn't reach their ends.
There are 2 independent parts, one for each index of `clips`. The reference program is written for one: setup_inputs(seed, part) draws one part's arguments, and reference() takes and returns one part's arrays. A program takes and returns all parts, laid end to end along the dimension named above; an argument that names none is the same for every part. Nothing has to cross between parts.
Inputs may be any that keep to these rules, and one draw needn't show every extreme that they name: `tile_list`: row b names tile b first, then tile_count[b] - 1 distinct other tiles within 4 of b; the remaining entries are -1. `tile_count`: some block lists 5 tiles.
All inputs are finite; a program needn't handle non-finite values.
Results may differ from the reference program's by a relative error of at most 0.014.
Values may be sent and summed in bfloat16 or wider, within the bound.
A program may use at most 64 MiB of HBM per device.

```python
import jax
import jax.numpy as jnp
from jax import lax

H = 12
HD = 128
D = 1536
TOK_DEV = 128
AUD_DEV = 8
RMAX = 2
SPAN = 4
LMAX = 5
TILES = 16
NV = 2048
NA = 128


def key_field(key):
    drawn = jnp.clip(jax.random.normal(jax.random.fold_in(key, 101), (NV, D), jnp.float32), -6.0, 6.0)
    return drawn


def draw_video_k(key, part):
    return key_field(key).astype(jnp.bfloat16)


def draw_video_q(key, part):
    drawn = jnp.clip(jax.random.normal(jax.random.fold_in(key, 103), (NV, D), jnp.float32), -6.0, 6.0)
    return drawn.astype(jnp.bfloat16)


def draw_audio_q(key, part):
    drawn = jnp.clip(jax.random.normal(jax.random.fold_in(key, 106), (NA, D), jnp.float32), -6.0, 6.0)
    return drawn.astype(jnp.bfloat16)


def tile_tables(key):
    base_key = jax.random.fold_in(key, 201)
    block_counts = jax.random.randint(jax.random.fold_in(base_key, 1), (TILES,), 1, LMAX + 1)
    full_block = jax.random.randint(jax.random.fold_in(base_key, 2), (), 0, TILES)
    block_counts = jnp.where(jnp.arange(TILES) == full_block, LMAX, block_counts).astype(jnp.int32)
    candidate_offsets = jnp.concatenate([jnp.arange(-SPAN, 0), jnp.arange(1, SPAN + 1)])
    blocks = jnp.arange(TILES)[:, None]
    candidate = blocks + candidate_offsets[None, :]
    usable = (candidate >= 0) & (candidate < TILES)
    width_index = jnp.arange(2 * SPAN)[None, :]
    random_score = jax.random.randint(jax.random.fold_in(base_key, 3), (TILES, 2 * SPAN), 0, 1024) * 64 + width_index
    rank_score = jnp.where(usable, random_score, (1 << 20) + width_index)
    ordering = jnp.argsort(rank_score, axis=1, stable=True)
    picked = jnp.take_along_axis(candidate, ordering[:, :LMAX - 1], axis=1)
    tile_rows = jnp.concatenate([blocks, picked], axis=1)
    tile_rows = jnp.where(jnp.arange(LMAX)[None, :] < block_counts[:, None], tile_rows, -1)
    return (tile_rows.astype(jnp.int32), block_counts)


def draw_tile_list(key, part):
    return tile_tables(key)[0]


def draw_tile_count(key, part):
    return tile_tables(key)[1]


def place_ends(values, rng, smallest, high):
    dims = values.shape
    place = [jax.random.randint(jax.random.fold_in(rng, axis), (), 0, dims[axis]) for axis in range(len(dims))]
    values = values.at[tuple(place)].set(smallest)
    longest = dims.index(max(dims))
    place[longest] = (place[longest] + 1) % dims[longest]
    return values.at[tuple(place)].set(high)


def levels(rng, extent, split, least, high):
    loudness = 1.0
    for axis_at, shards_of in split:
        steps = jax.random.uniform(jax.random.fold_in(jax.random.fold_in(rng, 6), axis_at), (shards_of,), jnp.float32, least / len(split), high / len(split))
        loudness = loudness * jnp.repeat(jnp.exp(steps), extent[axis_at] // shards_of).reshape((-1,) + (1,) * (len(extent) - 1 - axis_at))
    return loudness


def centred(rng, extent, deviation, most, cuts=(), held_as=jnp.bfloat16):
    values = jax.random.normal(rng, extent, jnp.float32) * deviation
    if len(cuts) > 0:
        values = levels(rng, extent, cuts, -0.22, 0.18) * values
    return jnp.clip(values, min=-most, max=most).astype(held_as)


def setup_inputs(seed: int = 0, part: int = 0) -> dict:
    arg_keys = jax.random.split(jax.random.key(seed), 12)
    part_keys = jax.random.split(jax.random.fold_in(arg_keys[11], part), 12)
    video_q = draw_video_q(jax.random.fold_in(jax.random.fold_in(arg_keys[11], part), 71), part)
    video_k = draw_video_k(jax.random.fold_in(jax.random.fold_in(arg_keys[11], part), 71), part)
    video_v = centred(part_keys[2], (NV, D), 1.0, 6.0, ((0, 16),))
    audio_q = draw_audio_q(jax.random.fold_in(jax.random.fold_in(arg_keys[11], part), 71), part)
    audio_k = centred(part_keys[4], (NA, D), 1.0, 6.0, ((0, 16),))
    audio_v = centred(part_keys[5], (NA, D), 1.0, 6.0, ((0, 16),))
    radius = place_ends(jax.random.randint(part_keys[6], (TILES,), 1, RMAX + 1), jax.random.fold_in(part_keys[6], 1), 1, RMAX).astype(jnp.int32)
    tile_list = draw_tile_list(jax.random.fold_in(jax.random.fold_in(arg_keys[11], part), 71), part)
    tile_count = draw_tile_count(jax.random.fold_in(jax.random.fold_in(arg_keys[11], part), 71), part)
    video_gain = jnp.clip(1.0 + 0.1 * jax.random.normal(arg_keys[9], (D,), jnp.float32), 0.5, 1.5)
    audio_gain = jnp.clip(1.0 + 0.1 * jax.random.normal(arg_keys[10], (D,), jnp.float32), 0.5, 1.5)
    return dict(video_q=video_q, video_k=video_k, video_v=video_v, audio_q=audio_q, audio_k=audio_k, audio_v=audio_v, radius=radius, tile_list=tile_list, tile_count=tile_count, video_gain=video_gain, audio_gain=audio_gain)


negative_big = -1e+30
epsilon = 1e-06

def split_heads(matrix):
    return matrix.astype(jnp.float32).reshape(matrix.shape[0], H, HD)

def softmax_attend(queries, key_rows, value_rows, key_valid):
    scores = jnp.einsum('qhd,khd->hqk', split_heads(queries), split_heads(key_rows)) * HD ** (-0.5)
    scores = jnp.where(key_valid[None, None, :], scores, negative_big)
    row_peak = lax.optimization_barrier(jnp.max(scores, axis=-1, keepdims=True))
    weights = jnp.exp(scores - row_peak).astype(jnp.bfloat16)
    weights = lax.optimization_barrier(weights).astype(jnp.float32)
    weight_sum = lax.optimization_barrier(jnp.sum(weights, axis=-1))
    mixed = jnp.einsum('hqk,khd->hqd', weights, split_heads(value_rows)) / weight_sum[..., None]
    return jnp.transpose(mixed, (1, 0, 2)).reshape(queries.shape[0], H * HD)

def rms_scale(mixed, gain):
    mean_square = lax.optimization_barrier(jnp.mean(mixed * mixed, axis=-1, keepdims=True))
    return (mixed * lax.rsqrt(mean_square + epsilon) * gain.astype(jnp.float32)).astype(jnp.bfloat16)

def reference(video_q, video_k, video_v, audio_q, audio_k, audio_v, radius, tile_list, tile_count, video_gain, audio_gain):
    span_tiles = 2 * RMAX + 1
    key_tiles = jnp.pad(video_k.reshape(TILES, TOK_DEV, D), ((RMAX, RMAX), (0, 0), (0, 0)))
    value_tiles = jnp.pad(video_v.reshape(TILES, TOK_DEV, D), ((RMAX, RMAX), (0, 0), (0, 0)))
    query_tiles = video_q.reshape(TILES, TOK_DEV, D)
    offsets = jnp.arange(-RMAX, RMAX + 1, dtype=jnp.int32)

    def video_tile(tile_index):
        start = (tile_index, jnp.int32(0), jnp.int32(0))
        window_keys = lax.dynamic_slice(key_tiles, start, (span_tiles, TOK_DEV, D)).reshape(span_tiles * TOK_DEV, D)
        window_values = lax.dynamic_slice(value_tiles, start, (span_tiles, TOK_DEV, D)).reshape(span_tiles * TOK_DEV, D)
        neighbour = tile_index + offsets
        tile_valid = (jnp.abs(offsets) <= radius[tile_index]) & (neighbour >= 0) & (neighbour < TILES)
        key_valid = jnp.concatenate([jnp.repeat(tile_valid, TOK_DEV), jnp.ones((NA,), dtype=bool)])
        key_rows = jnp.concatenate([window_keys, audio_k], axis=0)
        value_rows = jnp.concatenate([window_values, audio_v], axis=0)
        queries = lax.dynamic_index_in_dim(query_tiles, tile_index, 0, keepdims=False)
        return softmax_attend(queries, key_rows, value_rows, key_valid)
    video_mixed = lax.map(video_tile, jnp.arange(TILES, dtype=jnp.int32))
    video_out = rms_scale(video_mixed.reshape(NV, D), video_gain)
    audio_tiles = audio_q.reshape(TILES, AUD_DEV, D)
    video_key_tiles = video_k.reshape(TILES, TOK_DEV, D)
    video_value_tiles = video_v.reshape(TILES, TOK_DEV, D)

    def audio_block(block_index):
        listed = tile_list[block_index]
        chosen = jnp.maximum(listed, 0).astype(jnp.int32)
        key_rows = video_key_tiles[chosen].reshape(LMAX * TOK_DEV, D)
        value_rows = video_value_tiles[chosen].reshape(LMAX * TOK_DEV, D)
        entry_valid = jnp.arange(LMAX, dtype=jnp.int32) < tile_count[block_index]
        key_valid = jnp.repeat(entry_valid, TOK_DEV)
        queries = lax.dynamic_index_in_dim(audio_tiles, block_index, 0, keepdims=False)
        return softmax_attend(queries, key_rows, value_rows, key_valid)
    audio_mixed = lax.map(audio_block, jnp.arange(TILES, dtype=jnp.int32))
    audio_out = rms_scale(audio_mixed.reshape(NA, D), audio_gain)
    return (video_out, audio_out)
```

```python
import contextlib
import functools

import jax
import jax.numpy as jnp
from jax import lax
from jax.experimental import pallas as pl
from jax.experimental.pallas import tpu as pltpu
from jax.sharding import PartitionSpec as P

HD = 128
RMAX = 2
SPAN = 4
LOG2E = 1.4426950408889634
SCALE = HD ** (-0.5) * LOG2E
NEG = -1e30
EPS = 1e-6
MESH = pl.DeviceIdType.MESH
LAG_Z = 4
LAG_C = 6
FAR_STEPS = 4
COLUMN_1 = 1
COLUMN_2 = 4
COLUMN_3 = 8
CATCH_UP = 5
PAIR = 2
OWN_FIRST = 2


def part(name):
    return contextlib.nullcontext()


def kernel(
    n, heads, tok, aud, lmax,
    radius_hbm, tile_list_hbm, tile_count_hbm,
    vq_hbm, vk_hbm, vv_hbm, aq_hbm, ak_hbm, av_hbm, vgain_hbm, again_hbm,
    attn, aattn, vgain, again,
    radius, tile_list, tile_count,
    kv, audio, qown, aqown, aqin, qx, qr, part_o, part_s, back_o, back_s, tops, sums, atops, asums,
    load_sem, own_sem, s_kv, r_dk, r_y, s_z, r_z, r_d,
    s_col, r_col, s_aud, r_across, r_daud, s_q, r_q, s_bo, r_bo, s_bs, r_bs,
):
    me = lax.axis_index("seq")
    chips = n // 2
    chip = me // 2
    core = me % 2
    mate = chip * 2 + (1 - core)
    odd = chip % 2
    across_chip = chip + 1 - 2 * odd
    across = across_chip * 2 + core
    step = 2 - 4 * odd
    fwd_chip = chip + step
    has_fwd = (fwd_chip >= 0) & (fwd_chip < chips)
    src_chip = chip - step
    has_src = (src_chip >= 0) & (src_chip < chips)
    zchip = chip - 1 + 2 * odd
    fwd = jnp.clip(fwd_chip, 0, chips - 1) * 2 + core

    barrier = pltpu.get_barrier_semaphore()

    def greet(device):
        pl.semaphore_signal(barrier, inc=1, device_id={"seq": device}, device_id_type=MESH)

    low, high = chip >= 2, chip + 2 < chips
    up_to = jnp.clip(chip + 2, 0, chips - 1) * 2 + core
    down_to = jnp.clip(chip - 2, 0, chips - 1) * 2 + core
    greet(across)
    greet(mate)
    for exists, device in ((high, up_to), (low, down_to)):
        @pl.when(exists)
        def _(device=device):
            greet(device)

    loads = [
        pltpu.make_async_copy(aq_hbm, aqown, load_sem.at[0]),
        pltpu.make_async_copy(ak_hbm, audio.at[me, 0], load_sem.at[1]),
        pltpu.make_async_copy(av_hbm, audio.at[me, 1], load_sem.at[1]),
        pltpu.make_async_copy(vq_hbm, qown, load_sem.at[2]),
        pltpu.make_async_copy(vgain_hbm, vgain, load_sem.at[3]),
        pltpu.make_async_copy(again_hbm, again, load_sem.at[4]),
        pltpu.make_async_copy(radius_hbm, radius, load_sem.at[5]),
        pltpu.make_async_copy(tile_list_hbm, tile_list, load_sem.at[6]),
        pltpu.make_async_copy(tile_count_hbm, tile_count, load_sem.at[7]),
    ]

    def cols(h):
        return pl.ds(pl.multiple_of(h * HD, HD), HD)

    def own_head(h):
        return [
            pltpu.make_async_copy(side.at[:, cols(h)], kv.at[h, j, pl.ds(0, tok)], own_sem.at[jnp.minimum(h, OWN_FIRST)])
            for j, side in enumerate((vk_hbm, vv_hbm))
        ]

    for load in loads[:3]:
        load.start()

    def load_own(h, _):
        for load in own_head(h):
            load.start()
        return 0

    lax.fori_loop(0, heads, load_own, 0)
    for load in loads[3:]:
        load.start()

    @pl.when(jnp.logical_not(has_src))
    def _():
        def clear(h, _):
            kv[h, :, pl.ds(3 * tok, tok), :] = jnp.zeros((2, tok, HD), kv.dtype)
            return 0

        lax.fori_loop(0, heads, clear, 0)

    far = [(0, high, up_to), (1, low, down_to)]
    for slot, exists, device in far:
        @pl.when(jnp.logical_not(exists))
        def _(slot=slot):
            aqin[slot] = jnp.zeros(aqin.shape[1:], aqin.dtype)
            back_o[slot] = jnp.zeros(back_o.shape[1:], back_o.dtype)
            back_s[slot] = jnp.zeros(back_s.shape[1:], back_s.dtype)

    with part("barrier"):
        pl.semaphore_wait(barrier, 2 + high.astype(jnp.int32) + low.astype(jnp.int32))

    def remote(src, dst, s, r, device):
        return pltpu.make_async_remote_copy(
            src_ref=src, dst_ref=dst, send_sem=s, recv_sem=r,
            device_id={"seq": device}, device_id_type=MESH)

    def q_copy(slot, device):
        return remote(aqown, aqin.at[1 - slot], s_q.at[slot], r_q.at[1 - slot], device)

    def q_arrival(slot):
        return remote(aqown, aqin.at[slot], s_q.at[slot], r_q.at[slot], mate)

    row, rows_all = chip // 2, chips // 2

    def aud_copy(sem, landed, block, device):
        return remote(audio.at[block], audio.at[block], sem, landed, device)

    def daud_copy(block):
        return aud_copy(s_aud, r_daud, block, mate)

    def spread_up(block):
        return aud_copy(s_col, r_col.at[block // 4], block, up_to)

    def spread_down(block):
        return aud_copy(s_col, r_col.at[block // 4], block, down_to)

    def spread_across(block):
        return aud_copy(s_aud, r_across, block, across)

    def from_below(d, act):
        @pl.when(row - d >= 0)
        def _():
            block = jnp.maximum(me - 4 * d, 0)
            act(block)

    def from_above(d, act):
        @pl.when(row + d < rows_all)
        def _():
            block = jnp.minimum(me + 4 * d, n - 1)
            act(block)

    def column_step(d):
        def below(block):
            spread_up(block).wait_recv()

            @pl.when(high)
            def _():
                spread_up(block).start()
            spread_across(block).start()
            daud_copy(block).start()

        def above(block):
            spread_down(block).wait_recv()

            @pl.when(low)
            def _():
                spread_down(block).start()
            spread_across(block).start()
            daud_copy(block).start()

        from_below(d, below)
        from_above(d, above)

    def several(count, sem):
        blocks = audio.at[pl.ds(0, count)]
        return remote(blocks, blocks, sem, sem, mate)

    def pass_audio():
        several(rows_all, r_across).wait_recv()

        def forward(i, _):
            daud_copy(4 * i + across % 4).start()
            return 0

        lax.fori_loop(0, rows_all, forward, 0)

    def take_audio():
        several(chips, r_daud).wait_recv()

    def kv_head(slot, h):
        return kv.at[h, :, pl.ds(slot * tok, tok)]

    def y_copy(h):
        return remote(kv_head(0, h), kv_head(2, h), s_kv, r_y.at[h], across)

    def z_copy(h):
        return remote(kv_head(2, h), kv_head(3, h), s_z, r_z.at[h], fwd)

    def d_copy(h):
        return remote(kv.at[h, :, pl.ds(2 * tok, 2 * tok)], kv.at[h, :, pl.ds(4 * tok, 2 * tok)], s_kv, r_d.at[h], mate)

    dk = remote(kv.at[:, :, pl.ds(0, tok)], kv.at[:, :, pl.ds(tok, tok)], s_kv, r_dk, mate)

    def own_there(first, count):
        there = kv.at[pl.ds(first, count), :, pl.ds(0, tok)]
        pltpu.make_async_copy(there, there, own_sem.at[min(first, OWN_FIRST)]).wait()

    for h in range(OWN_FIRST):
        own_there(h, 1)
        y_copy(h).start()
    loads[0].wait()
    for slot, exists, device in far:
        @pl.when(exists)
        def _(slot=slot, device=device):
            q_copy(slot, device).start()
    pltpu.make_async_copy(audio.at[me], audio.at[me], load_sem.at[1]).wait()

    @pl.when(high)
    def _():
        spread_up(me).start()

    @pl.when(low)
    def _():
        spread_down(me).start()
    own_there(OWN_FIRST, heads - OWN_FIRST)
    for h in range(OWN_FIRST, heads):
        y_copy(h).start()
    spread_across(me).start()
    daud_copy(me).start()
    dk.start()

    for load in loads[3:9]:
        load.wait()
    wide = jnp.concatenate([aqown[...].astype(jnp.float32), jnp.zeros((aud, heads * HD), jnp.float32)], axis=0)
    qx[...] = wide.astype(jnp.bfloat16)

    def dot_t(a, b):
        return lax.dot_general(a, b, (((1,), (1,)), ((), ())), preferred_element_type=jnp.float32)

    def is_listed(block, tile):
        listed = jnp.int32(0)
        for j in range(lmax):
            listed = jnp.where((tile_list[j, block] == tile) & (j < tile_count[block]), 1, listed)
        return listed > 0

    def bias_of(seen):
        return jnp.where(seen, 0.0, NEG).astype(jnp.float32)

    tiles = [me, mate, across, zchip * 2 + core, across_chip * 2 + 1 - core, zchip * 2 + 1 - core]
    near = radius[0]
    see_v, see_a = [], []
    for tile in tiles:
        inside = (tile >= 0) & (tile < n)
        see_v.append(bias_of(inside & (jnp.abs(tile - me) <= near)))
        see_a.append(bias_of(inside & is_listed(me, tile)))
    upper = lax.broadcasted_iota(jnp.int32, (2 * aud, tok), 0) < aud
    see_far = [
        jnp.where(upper, bias_of(is_listed(up_to, tile)), bias_of(is_listed(down_to, tile)))
        for tile in (me, mate)
    ]
    far_there = [bias_of(exists) for _, exists, _ in far]

    lane = lax.broadcasted_iota(jnp.int32, (aud, HD), 1)

    def far_group(hs):
        loaded = [(qr[:, cols(h)], kv[h, 0, pl.ds(0, 2 * tok)], kv[h, 1, pl.ds(0, 2 * tok)]) for h in hs]
        scores = [dot_t(q, k) for q, k, _ in loaded]
        results = []
        for s, (_, _, v) in zip(scores, loaded):
            sides = [s[:, j * tok:(j + 1) * tok] * SCALE + see_far[j] for j in range(2)]
            m = jnp.max(jnp.maximum(*sides), axis=1, keepdims=True)
            w = jnp.concatenate([jnp.exp2(side - m).astype(jnp.bfloat16) for side in sides], axis=1)
            ones = jnp.ones((2 * tok, HD), jnp.bfloat16)
            results.append((m, jnp.dot(w, jnp.concatenate([v, ones], axis=1), preferred_element_type=jnp.float32)))
        stats = [part_s[slot] for slot in range(2)]
        for h, (m, o) in zip(hs, results):
            mean = (o[:, :HD] / o[:, HD:]).astype(part_o.dtype).astype(jnp.float32)
            for slot in range(2):
                rows = slice(slot * aud, (slot + 1) * aud)
                part_o[slot, :, cols(h)] = mean[rows].astype(part_o.dtype)
                stats[slot] = jnp.where(lane == h, m[rows], stats[slot])
                stats[slot] = jnp.where(lane == h + 64, o[rows, HD:], stats[slot])
        for slot in range(2):
            part_s[slot] = stats[slot]

    def bo_copy(slot, device):
        return remote(part_o.at[slot], back_o.at[1 - slot], s_bo.at[slot], r_bo.at[1 - slot], device)

    def bs_copy(slot, device):
        return remote(part_s.at[slot], back_s.at[1 - slot], s_bs.at[slot], r_bs.at[1 - slot], device)

    def far_open():
        dk.wait_recv()
        for slot, exists, device in far:
            @pl.when(exists)
            def _(slot=slot):
                q_arrival(slot).wait_recv()
        both = jnp.concatenate([aqin[0].astype(jnp.float32), aqin[1].astype(jnp.float32)], axis=0)
        qr[...] = both.astype(jnp.bfloat16)
        part_s[...] = jnp.zeros(part_s.shape, jnp.float32)

    far_each = -(-heads // FAR_STEPS)

    def far_some(i):
        far_group([jnp.minimum(i * far_each + j, heads - 1) for j in range(far_each)])

    def far_close():
        for slot, exists, device in far:
            @pl.when(exists)
            def _(slot=slot, device=device):
                bo_copy(slot, device).start()
                bs_copy(slot, device).start()

    def lay_audio(i, _):
        for j in range(2):
            pair = jnp.concatenate(
                [audio[2 * i, j].astype(jnp.float32), audio[2 * i + 1, j].astype(jnp.float32)], axis=0)
            pair = pair.astype(jnp.bfloat16)
            for h in range(heads):
                kv[h, j, pl.ds(pl.multiple_of(6 * tok + 2 * aud * i, 2 * aud), 2 * aud), :] = pair[:, h * HD:(h + 1) * HD]
        return 0

    span = 6 * tok
    keys = span + n * aud

    def softmax_part(s, biases):
        blocks = [s[:, i * tok:(i + 1) * tok] * SCALE + biases[i] for i in range(len(biases))]
        if s.shape[1] > len(biases) * tok:
            blocks.append(s[:, len(biases) * tok:] * SCALE)
        m = functools.reduce(jnp.maximum, [jnp.max(b, axis=1, keepdims=True) for b in blocks]) if blocks[-1].shape[1] != tok else jnp.max(functools.reduce(jnp.maximum, blocks), axis=1, keepdims=True)
        w = jnp.concatenate([jnp.exp2(b - m).astype(jnp.bfloat16) for b in blocks], axis=1)
        return m, w

    def merge(h, oa, la, ma, stats, far_o):
        peaks, totals = [], []
        for slot in range(2):
            st = stats[slot]
            peaks.append(jnp.max(jnp.where(lane == h, st, NEG), axis=1, keepdims=True) + far_there[slot])
            totals.append(jnp.sum(jnp.where(lane == h + 64, st, 0.0), axis=1, keepdims=True))
        peak = functools.reduce(jnp.maximum, peaks, ma)
        shrink = jnp.exp2(ma - peak)
        oa = oa * shrink
        la = la * shrink
        for slot in range(2):
            share = jnp.exp2(peaks[slot] - peak) * totals[slot]
            oa = oa + far_o[slot].astype(jnp.float32) * share
            la = la + share
        return oa / la

    def far_back(hs):
        return [back_s[slot] for slot in range(2)], [[back_o[slot, :, cols(h)] for slot in range(2)] for h in hs]

    def mix(hs, width):
        qs = [jnp.concatenate([qown[:, cols(h)], qx[:, cols(h)]], axis=0) for h in hs]
        ks = [kv[h, 0, pl.ds(0, width)] for h in hs]
        vs = [jnp.concatenate([kv[h, 1, pl.ds(0, width)], jnp.ones((width, HD), jnp.bfloat16)], axis=1) for h in hs]
        scores = [dot_t(q, k) for q, k in zip(qs, ks)]
        weights = []
        for s in scores:
            mv, wv = softmax_part(s[:tok], see_v)
            ma, wa = softmax_part(s[tok:, :span], see_a)
            if width > span:
                wa = jnp.concatenate([wa, jnp.zeros((2 * aud, width - span), jnp.bfloat16)], axis=1)
            weights.append((mv, ma[:aud], jnp.concatenate([wv, wa], axis=0)))
        return [(mv, ma, jnp.dot(w, v, preferred_element_type=jnp.float32)) for (mv, ma, w), v in zip(weights, vs)]

    def heads_full(hs):
        stats, far_o = far_back(hs)
        mixed = mix(hs, keys)
        merged = [merge(h, o[tok:tok + aud, :HD], o[tok:tok + aud, HD:], ma, stats, f)
                  for h, (_, ma, o), f in zip(hs, mixed, far_o)]
        for h, (_, _, o), joined in zip(hs, mixed, merged):
            attn[:, cols(h)] = o[:tok, :HD] / o[:tok, HD:]
            aattn[:, cols(h)] = joined

    def heads_video(hs):
        for h, (mv, ma, o) in zip(hs, mix(hs, span)):
            attn[:, cols(h)] = o[:tok, :HD]
            sums[h] = o[:tok, HD:]
            tops[h] = jnp.broadcast_to(mv, (tok, HD))
            aattn[:, cols(h)] = o[tok:tok + aud, :HD]
            asums[h] = o[tok:tok + aud, HD:]
            atops[h] = jnp.broadcast_to(ma, (aud, HD))

    def heads_audio(hs):
        stats, far_o = far_back(hs)
        loaded = [
            (qown[:, cols(h)], kv[h, 0, pl.ds(span, n * aud)],
             jnp.concatenate([kv[h, 1, pl.ds(span, n * aud)], jnp.ones((n * aud, HD), jnp.bfloat16)], axis=1))
            for h in hs]
        held = [(attn[:, cols(h)], sums[h], tops[h], aattn[:, cols(h)], asums[h], atops[h]) for h in hs]
        scores = [dot_t(q, k) * SCALE for q, k, _ in loaded]
        peaks = [jnp.maximum(jnp.max(s, axis=1, keepdims=True), top) for s, (_, _, top, _, _, _) in zip(scores, held)]
        mixed = [
            jnp.dot(jnp.exp2(s - peak[:, :1]).astype(jnp.bfloat16), v, preferred_element_type=jnp.float32)
            for s, peak, (_, _, v) in zip(scores, peaks, loaded)]
        merged = [merge(h, oa, la, ma, stats, f) for h, (_, _, _, oa, la, ma), f in zip(hs, held, far_o)]
        for h, o, peak, (old, total, top, _, _, _), joined in zip(hs, mixed, peaks, held, merged):
            shrink = jnp.exp2(top - peak)
            attn[:, cols(h)] = (old * shrink + o[:, :HD]) / (total * shrink + o[:, HD:])
            aattn[:, cols(h)] = joined

    def sent():
        for slot, exists, device in far:
            @pl.when(exists)
            def _(slot=slot, device=device):
                q_copy(slot, device).wait_send()
                bo_copy(slot, device).wait_send()
                bs_copy(slot, device).wait_send()

        @pl.when(high & low)
        def _():
            several(rows_all + 1, s_col).wait_send()

        @pl.when(high != low)
        def _():
            several(1, s_col).wait_send()
        several(3 * rows_all, s_aud).wait_send()

    audio_ready = heads + LAG_Z - 1
    early = heads // PAIR - 1

    def relay(i, _):
        @pl.when(i < heads)
        def _():
            with part("ywait"):
                y_copy(i).wait_recv()

            @pl.when(has_fwd)
            def _():
                z_copy(i).start()


        @pl.when((i >= LAG_Z) & (i < heads + LAG_Z))
        def _():
            @pl.when(has_src)
            def _():
                with part("zwait"):
                    z_copy(i - LAG_Z).wait_recv()
            d_copy(i - LAG_Z).start()

        @pl.when(i == COLUMN_1)
        def _():
            with part("col1"):
                column_step(1)

        @pl.when(i == 0)
        def _():
            with part("faropen"):
                far_open()

        @pl.when(i == COLUMN_2)
        def _():
            if rows_all > 2:
                with part("col2"):
                    column_step(2)

        @pl.when(i == COLUMN_3)
        def _():
            def more(d, _):
                column_step(d)
                return 0

            with part("col3"):
                lax.fori_loop(3, rows_all, more, 0)

        @pl.when(i < FAR_STEPS)
        def _():
            with part("far"):
                far_some(i)

        @pl.when(i == FAR_STEPS - 1)
        def _():
            far_close()

        @pl.when(i == audio_ready - 1)
        def _():
            with part("passaudio"):
                pass_audio()

        @pl.when(i == audio_ready)
        def _():
            with part("takeaudio"):
                take_audio()
            with part("layaudio"):
                lax.fori_loop(0, chips, lay_audio, 0)
            with part("bowait"):
                for slot, exists, device in far:
                    @pl.when(exists)
                    def _(slot=slot):
                        bo_copy(1 - slot, mate).wait_recv()
                        bs_copy(1 - slot, mate).wait_recv()
            with part("sent"):
                sent()

        def arrive(hs):
            with part("dwait"):
                for h in hs:
                    d_copy(h).wait_recv()

        def attend_video(p, _):
            hs = [p * PAIR + k for k in range(PAIR)]
            arrive(hs)
            with part("vhead"):
                heads_video(hs)
            return 0

        def attend_audio(g, _):
            with part("ahead"):
                heads_audio([g * CATCH_UP + k for k in range(CATCH_UP)])
            return 0

        def attend(p, _):
            hs = [p * PAIR + k for k in range(PAIR)]
            arrive(hs)
            with part("head"):
                heads_full(hs)
            return 0

        lax.fori_loop(jnp.minimum(pairs(i - 1), early), jnp.minimum(pairs(i), early), attend_video, 0)
        lax.fori_loop(caught(i - 1), caught(i), attend_audio, 0)
        lax.fori_loop(jnp.maximum(pairs(i - 1), early), jnp.maximum(pairs(i), early), attend, 0)
        return 0

    def pairs(i):
        due = jnp.where(i < heads, i - LAG_C + 1, jnp.where(i <= audio_ready, i - LAG_Z, heads))
        return jnp.clip(due // PAIR, 0, heads // PAIR)

    def caught(i):
        return jnp.clip(early * PAIR * (i - audio_ready + 1) // CATCH_UP, 0, early * PAIR // CATCH_UP)

    lax.fori_loop(0, heads + LAG_Z + 1, relay, 0)

    with part("drain"):
        kv_sent = kv.at[:, :, pl.ds(0, 4 * tok)]
        remote(kv_sent, kv_sent, s_kv, r_dk, mate).wait_send()

        @pl.when(has_fwd)
        def _():
            z_sent = kv.at[:, :, pl.ds(0, tok)]
            remote(z_sent, z_sent, s_z, r_dk, mate).wait_send()


def finish_kernel(attn, aattn, vgain, again, vout, aout):
    def finish(mixed, gain):
        scale = lax.rsqrt(jnp.mean(mixed * mixed, axis=1, keepdims=True) + EPS)
        return (mixed * scale * gain[...].reshape(1, mixed.shape[1])).astype(jnp.bfloat16)

    vout[...] = finish(attn[...], vgain)
    aout[...] = finish(aattn[...], again)


def solution(mesh):
    n = mesh.shape["seq"]
    chips = n // 2

    def on_device(vq, vk, vv, aq, ak, av, radius, tile_list, tile_count, vgain, again):
        tok, width = vq.shape
        aud = aq.shape[0]
        heads = width // HD
        keys = 6 * tok + n * aud
        bf, f32 = jnp.bfloat16, jnp.float32
        dma = pltpu.SemaphoreType.DMA
        per_head = dma((heads,))
        hbm = pl.BlockSpec(memory_space=pltpu.HBM)
        vmem = pl.BlockSpec(memory_space=pltpu.VMEM)
        mixed = pl.pallas_call(
            functools.partial(kernel, n, heads, tok, aud, tile_list.shape[1]),
            out_shape=(
                pltpu.VMEM((tok, width), f32), pltpu.VMEM((aud, width), f32),
                pltpu.VMEM((width,), f32), pltpu.VMEM((width,), f32),
            ),
            in_specs=[hbm] * 11,
            out_specs=(vmem,) * 4,
            scratch_shapes=[
                pltpu.SMEM(radius.shape, jnp.int32),
                pltpu.SMEM(tile_list.shape[::-1], jnp.int32),
                pltpu.SMEM(tile_count.shape, jnp.int32),
                pltpu.VMEM((heads, 2, keys, HD), bf),
                pltpu.VMEM((n, 2, aud, width), bf),
                pltpu.VMEM((tok, width), bf),
                pltpu.VMEM((aud, width), bf),
                pltpu.VMEM((2, aud, width), bf),
                pltpu.VMEM((2 * aud, width), bf),
                pltpu.VMEM((2 * aud, width), bf),
                pltpu.VMEM((2, aud, width), bf),
                pltpu.VMEM((2, aud, HD), f32),
                pltpu.VMEM((2, aud, width), bf),
                pltpu.VMEM((2, aud, HD), f32),
                *([pltpu.VMEM((heads, tok, HD), f32)] * 2),
                *([pltpu.VMEM((heads, aud, HD), f32)] * 2),
                dma((8,)), dma((OWN_FIRST + 1,)), dma, dma,
                per_head, dma, per_head, per_head,
                dma, dma((chips // 2,)), dma, dma, dma,
                *([dma((2,))] * 6),
            ],
            compiler_params=pltpu.CompilerParams(
                collective_id=0, has_side_effects=True),
        )(radius, tile_list.T, tile_count, vq, vk, vv, aq, ak, av, vgain, again)
        return pl.pallas_call(
            finish_kernel,
            out_shape=(jax.ShapeDtypeStruct(vq.shape, bf), jax.ShapeDtypeStruct(aq.shape, bf)),
            in_specs=[vmem] * 4,
            out_specs=(vmem, vmem),
            compiler_params=pltpu.CompilerParams(vmem_limit_bytes=8 * 1024 * 1024),
        )(*mixed)

    rows = P(("clips", "seq"), None)
    return jax.shard_map(
        on_device,
        mesh=mesh,
        in_specs=(rows,) * 6 + (P(("clips", "seq")), P("clips", None), P("clips"), P(), P()),
        out_specs=(rows, rows),
        check_vma=False,
    )
```

```python
import contextlib
import functools

import jax
import jax.numpy as jnp
from jax import lax
from jax.experimental import pallas as pl
from jax.experimental.pallas import tpu as pltpu
from jax.sharding import PartitionSpec as P

HD = 128
RMAX = 2
SPAN = 4
LOG2E = 1.4426950408889634
SCALE = HD ** (-0.5) * LOG2E
NEG = -1e30
EPS = 1e-6
MESH = pl.DeviceIdType.MESH
LAG_Z = 4
FAR_STEPS = 4
WAVES = (1, 4, 6, 8)
BESIDE = 9
WINDOW = 4
FIRST_PIECES = 2
LAST_PIECES = 4
MAIN_PAIRS = 3
CATCH_UP = 5
PAIR = 2
OWN_FIRST = 2


def part(name):
    return contextlib.nullcontext()


def kernel(
    n, heads, tok, aud, lmax,
    radius_hbm, tile_list_hbm, tile_count_hbm,
    vq_hbm, vk_hbm, vv_hbm, aq_hbm, ak_hbm, av_hbm, vgain_hbm, again_hbm,
    attn, aattn, vgain, again,
    radius, tile_list, tile_count,
    kv, audio, qown, aqown, aqin, qx, qr, part_o, part_s, back_o, back_s, tops, sums, atops, asums,
    load_sem, own_sem, s_kv, r_dk, r_y, s_z, r_z, r_d,
    s_link, r_aud, s_aud, r_daud, s_q, r_q, s_bo, r_bo, s_bs, r_bs,
):
    me = lax.axis_index("seq")
    chips = n // 2
    chip = me // 2
    core = me % 2
    mate = chip * 2 + (1 - core)
    odd = chip % 2
    across_chip = chip + 1 - 2 * odd
    across = across_chip * 2 + core
    step = 2 - 4 * odd
    fwd_chip = chip + step
    has_fwd = (fwd_chip >= 0) & (fwd_chip < chips)
    src_chip = chip - step
    has_src = (src_chip >= 0) & (src_chip < chips)
    zchip = chip - 1 + 2 * odd
    fwd = jnp.clip(fwd_chip, 0, chips - 1) * 2 + core

    barrier = pltpu.get_barrier_semaphore()

    def greet(device):
        pl.semaphore_signal(barrier, inc=1, device_id={"seq": device}, device_id_type=MESH)

    low, high = chip >= 2, chip + 2 < chips
    up_to = jnp.clip(chip + 2, 0, chips - 1) * 2 + core
    down_to = jnp.clip(chip - 2, 0, chips - 1) * 2 + core
    greet(across)
    greet(mate)
    for exists, device in ((high, up_to), (low, down_to)):
        @pl.when(exists)
        def _(device=device):
            greet(device)

    loads = [
        pltpu.make_async_copy(aq_hbm, aqown, load_sem.at[0]),
        pltpu.make_async_copy(ak_hbm, audio.at[me, 0], load_sem.at[1]),
        pltpu.make_async_copy(av_hbm, audio.at[me, 1], load_sem.at[1]),
        pltpu.make_async_copy(vq_hbm, qown, load_sem.at[2]),
        pltpu.make_async_copy(vgain_hbm, vgain, load_sem.at[3]),
        pltpu.make_async_copy(again_hbm, again, load_sem.at[4]),
        pltpu.make_async_copy(radius_hbm, radius, load_sem.at[5]),
        pltpu.make_async_copy(tile_list_hbm, tile_list, load_sem.at[6]),
        pltpu.make_async_copy(tile_count_hbm, tile_count, load_sem.at[7]),
    ]

    def cols(h):
        return pl.ds(pl.multiple_of(h * HD, HD), HD)

    def own_head(h):
        return [
            pltpu.make_async_copy(side.at[:, cols(h)], kv.at[h, j, pl.ds(0, tok)], own_sem.at[jnp.minimum(h, OWN_FIRST)])
            for j, side in enumerate((vk_hbm, vv_hbm))
        ]

    for load in loads[:3]:
        load.start()

    def load_own(h, _):
        for load in own_head(h):
            load.start()
        return 0

    lax.fori_loop(0, heads, load_own, 0)
    for load in loads[3:]:
        load.start()

    @pl.when(jnp.logical_not(has_src))
    def _():
        def clear(h, _):
            kv[h, :, pl.ds(3 * tok, tok), :] = jnp.zeros((2, tok, HD), kv.dtype)
            return 0

        lax.fori_loop(0, heads, clear, 0)

    far = [(0, high, up_to), (1, low, down_to)]
    for slot, exists, device in far:
        @pl.when(jnp.logical_not(exists))
        def _(slot=slot):
            aqin[slot] = jnp.zeros(aqin.shape[1:], aqin.dtype)
            back_o[slot] = jnp.zeros(back_o.shape[1:], back_o.dtype)
            back_s[slot] = jnp.zeros(back_s.shape[1:], back_s.dtype)

    with part("barrier"):
        pl.semaphore_wait(barrier, 2 + high.astype(jnp.int32) + low.astype(jnp.int32))

    def remote(src, dst, s, r, device):
        return pltpu.make_async_remote_copy(
            src_ref=src, dst_ref=dst, send_sem=s, recv_sem=r,
            device_id={"seq": device}, device_id_type=MESH)

    def q_copy(slot, device):
        return remote(aqown, aqin.at[1 - slot], s_q.at[slot], r_q.at[1 - slot], device)

    def q_arrival(slot):
        return remote(aqown, aqin.at[slot], s_q.at[slot], r_q.at[slot], mate)

    row, rows_all = chip // 2, chips // 2

    def aud_copy(sem, landed, block, device):
        return remote(audio.at[block], audio.at[block], sem, landed, device)

    def daud_copy(block):
        return aud_copy(s_aud, r_daud, block, mate)

    def link_copy(block, device):
        return aud_copy(s_link, r_aud.at[block // 2], block, device)

    turn = 1 - 2 * odd
    ahead = jnp.where(odd == 1, row, rows_all - 1 - row)
    behind = rows_all - 1 - ahead
    back = jnp.clip(src_chip, 0, chips - 1) * 2 + core

    def at_level(block, k):
        return jnp.clip(block + 4 * k * turn, 0, n - 1)

    def send_on(block):
        @pl.when(has_src)
        def _():
            link_copy(block, back).start()

    def to_front(block):
        @pl.when(has_fwd)
        def _():
            link_copy(block, fwd).start()

    def wave(first, k):
        @pl.when(k <= ahead)
        def _():
            block = at_level(first, k)
            link_copy(block, back).wait_recv()
            send_on(block)
            daud_copy(block).start()

            @pl.when(jnp.logical_not(has_src))
            def _():
                to_across(first, k)

    def to_across(first, k):
        @pl.when((k >= 2) & (k <= ahead))
        def _():
            link_copy(at_level(first, k), across).start()

    def wave_step(k):
        @pl.when(k == 0)
        def _():
            link_copy(across, back).wait_recv()
            send_on(across)
            to_front(across)
            daud_copy(across).start()

        @pl.when(k > 0)
        def _():
            wave(across, k)
        wave(me, k + 1)

    def from_behind(k):
        @pl.when(k <= behind)
        def _():
            for first in (me, across):
                block = at_level(first, -k)
                link_copy(block, across).wait_recv()
                daud_copy(block).start()

    def several(count, sem):
        blocks = audio.at[pl.ds(0, count)]
        return remote(blocks, blocks, sem, sem, mate)

    def pass_audio():
        def forward(k, _):
            from_behind(k)
            return 0

        lax.fori_loop(2, rows_all, forward, 0)

    def late_across():
        def send(k, _):
            to_across(me, k)
            to_across(across, k)
            return 0

        lax.fori_loop(2, rows_all, send, 0)

    def take_audio():
        several(chips, r_daud).wait_recv()

    def kv_head(slot, h):
        return kv.at[h, :, pl.ds(slot * tok, tok)]

    last = heads - 1

    def y_copy(h):
        return remote(kv_head(0, h), kv_head(2, h), s_kv, r_y.at[FIRST_PIECES + h - 1], across)

    def z_copy(h):
        return remote(kv_head(2, h), kv_head(3, h), s_z, r_z.at[FIRST_PIECES + h - 1], fwd)

    def pieces(h):
        return FIRST_PIECES if h == 0 else LAST_PIECES

    def piece(slot, h, p):
        count = tok // pieces(h)
        return kv.at[h, :, pl.ds(slot * tok + p * count, count)]

    def piece_sem(h, p):
        return (0 if h == 0 else FIRST_PIECES + heads - 2) + p

    def y_piece(h, p):
        return remote(piece(0, h, p), piece(2, h, p), s_kv, r_y.at[piece_sem(h, p)], across)

    def z_piece(h, p):
        return remote(piece(2, h, p), piece(3, h, p), s_z, r_z.at[piece_sem(h, p)], fwd)

    def d_copy(p):
        heads_of = pl.ds(PAIR * p, PAIR)
        return remote(
            kv.at[heads_of, :, pl.ds(2 * tok, 2 * tok)], kv.at[heads_of, :, pl.ds(4 * tok, 2 * tok)], s_kv, r_d.at[p], mate)

    dk = remote(kv.at[:, :, pl.ds(0, tok)], kv.at[:, :, pl.ds(tok, tok)], s_kv, r_dk, mate)

    def own_there(first, count):
        there = kv.at[pl.ds(first, count), :, pl.ds(0, tok)]
        pltpu.make_async_copy(there, there, own_sem.at[min(first, OWN_FIRST)]).wait()

    own_there(0, 1)
    for p in range(FIRST_PIECES):
        y_piece(0, p).start()
    pltpu.make_async_copy(audio.at[me], audio.at[me], load_sem.at[1]).wait()
    link_copy(me, across).start()
    for h in range(1, OWN_FIRST):
        own_there(h, 1)
        y_copy(h).start()
    loads[0].wait()
    for slot, exists, device in far:
        @pl.when(exists)
        def _(slot=slot, device=device):
            q_copy(slot, device).start()

    send_on(me)
    to_front(me)
    own_there(OWN_FIRST, heads - OWN_FIRST)
    for h in range(OWN_FIRST, WINDOW):
        y_copy(h).start()
    daud_copy(me).start()
    dk.start()

    for load in loads[3:9]:
        load.wait()
    wide = jnp.concatenate([aqown[...].astype(jnp.float32), jnp.zeros((aud, heads * HD), jnp.float32)], axis=0)
    qx[...] = wide.astype(jnp.bfloat16)

    def dot_t(a, b):
        return lax.dot_general(a, b, (((1,), (1,)), ((), ())), preferred_element_type=jnp.float32)

    def is_listed(block, tile):
        listed = jnp.int32(0)
        for j in range(lmax):
            listed = jnp.where((tile_list[j, block] == tile) & (j < tile_count[block]), 1, listed)
        return listed > 0

    def bias_of(seen):
        return jnp.where(seen, 0.0, NEG).astype(jnp.float32)

    tiles = [me, mate, across, zchip * 2 + core, across_chip * 2 + 1 - core, zchip * 2 + 1 - core]
    near = radius[0]
    see_v, see_a = [], []
    for tile in tiles:
        inside = (tile >= 0) & (tile < n)
        see_v.append(bias_of(inside & (jnp.abs(tile - me) <= near)))
        see_a.append(bias_of(inside & is_listed(me, tile)))
    upper = lax.broadcasted_iota(jnp.int32, (2 * aud, tok), 0) < aud
    see_far = [
        jnp.where(upper, bias_of(is_listed(up_to, tile)), bias_of(is_listed(down_to, tile)))
        for tile in (me, mate)
    ]
    far_there = [bias_of(exists) for _, exists, _ in far]

    lane = lax.broadcasted_iota(jnp.int32, (aud, HD), 1)

    def far_group(hs):
        loaded = [(qr[:, cols(h)], kv[h, 0, pl.ds(0, 2 * tok)], kv[h, 1, pl.ds(0, 2 * tok)]) for h in hs]
        scores = [dot_t(q, k) for q, k, _ in loaded]
        results = []
        for s, (_, _, v) in zip(scores, loaded):
            sides = [s[:, j * tok:(j + 1) * tok] * SCALE + see_far[j] for j in range(2)]
            m = jnp.max(jnp.maximum(*sides), axis=1, keepdims=True)
            w = jnp.concatenate([jnp.exp2(side - m).astype(jnp.bfloat16) for side in sides], axis=1)
            ones = jnp.ones((2 * tok, HD), jnp.bfloat16)
            results.append((m, jnp.dot(w, jnp.concatenate([v, ones], axis=1), preferred_element_type=jnp.float32)))
        stats = [part_s[slot] for slot in range(2)]
        for h, (m, o) in zip(hs, results):
            mean = (o[:, :HD] / o[:, HD:]).astype(part_o.dtype).astype(jnp.float32)
            for slot in range(2):
                rows = slice(slot * aud, (slot + 1) * aud)
                part_o[slot, :, cols(h)] = mean[rows].astype(part_o.dtype)
                stats[slot] = jnp.where(lane == h, m[rows], stats[slot])
                stats[slot] = jnp.where(lane == h + 64, o[rows, HD:], stats[slot])
        for slot in range(2):
            part_s[slot] = stats[slot]

    def bo_copy(slot, device):
        return remote(part_o.at[slot], back_o.at[1 - slot], s_bo.at[slot], r_bo.at[1 - slot], device)

    def bs_copy(slot, device):
        return remote(part_s.at[slot], back_s.at[1 - slot], s_bs.at[slot], r_bs.at[1 - slot], device)

    def far_open():
        dk.wait_recv()
        for slot, exists, device in far:
            @pl.when(exists)
            def _(slot=slot):
                q_arrival(slot).wait_recv()
        both = jnp.concatenate([aqin[0].astype(jnp.float32), aqin[1].astype(jnp.float32)], axis=0)
        qr[...] = both.astype(jnp.bfloat16)
        part_s[...] = jnp.zeros(part_s.shape, jnp.float32)

    far_each = -(-heads // FAR_STEPS)

    def far_some(i):
        far_group([jnp.minimum(i * far_each + j, heads - 1) for j in range(far_each)])

    def far_close():
        for slot, exists, device in far:
            @pl.when(exists)
            def _(slot=slot, device=device):
                bo_copy(slot, device).start()
                bs_copy(slot, device).start()

    def lay_audio(i, _):
        for j in range(2):
            pair = jnp.concatenate(
                [audio[2 * i, j].astype(jnp.float32), audio[2 * i + 1, j].astype(jnp.float32)], axis=0)
            pair = pair.astype(jnp.bfloat16)
            for h in range(heads):
                kv[h, j, pl.ds(pl.multiple_of(6 * tok + 2 * aud * i, 2 * aud), 2 * aud), :] = pair[:, h * HD:(h + 1) * HD]
        return 0

    span = 6 * tok
    keys = span + n * aud

    def softmax_part(s, biases):
        blocks = [s[:, i * tok:(i + 1) * tok] * SCALE + biases[i] for i in range(len(biases))]
        if s.shape[1] > len(biases) * tok:
            blocks.append(s[:, len(biases) * tok:] * SCALE)
        m = functools.reduce(jnp.maximum, [jnp.max(b, axis=1, keepdims=True) for b in blocks]) if blocks[-1].shape[1] != tok else jnp.max(functools.reduce(jnp.maximum, blocks), axis=1, keepdims=True)
        w = jnp.concatenate([jnp.exp2(b - m).astype(jnp.bfloat16) for b in blocks], axis=1)
        return m, w

    def merge(h, oa, la, ma, stats, far_o):
        peaks, totals = [], []
        for slot in range(2):
            st = stats[slot]
            peaks.append(jnp.max(jnp.where(lane == h, st, NEG), axis=1, keepdims=True) + far_there[slot])
            totals.append(jnp.sum(jnp.where(lane == h + 64, st, 0.0), axis=1, keepdims=True))
        peak = functools.reduce(jnp.maximum, peaks, ma)
        shrink = jnp.exp2(ma - peak)
        oa = oa * shrink
        la = la * shrink
        for slot in range(2):
            share = jnp.exp2(peaks[slot] - peak) * totals[slot]
            oa = oa + far_o[slot].astype(jnp.float32) * share
            la = la + share
        return oa / la

    def far_back(hs):
        return [back_s[slot] for slot in range(2)], [[back_o[slot, :, cols(h)] for slot in range(2)] for h in hs]

    def mix(hs, width):
        qs = [jnp.concatenate([qown[:, cols(h)], qx[:, cols(h)]], axis=0) for h in hs]
        ks = [kv[h, 0, pl.ds(0, width)] for h in hs]
        vs = [jnp.concatenate([kv[h, 1, pl.ds(0, width)], jnp.ones((width, HD), jnp.bfloat16)], axis=1) for h in hs]
        scores = [dot_t(q, k) for q, k in zip(qs, ks)]
        weights = []
        for s in scores:
            mv, wv = softmax_part(s[:tok], see_v)
            ma, wa = softmax_part(s[tok:, :span], see_a)
            if width > span:
                wa = jnp.concatenate([wa, jnp.zeros((2 * aud, width - span), jnp.bfloat16)], axis=1)
            weights.append((mv, ma[:aud], jnp.concatenate([wv, wa], axis=0)))
        return [(mv, ma, jnp.dot(w, v, preferred_element_type=jnp.float32)) for (mv, ma, w), v in zip(weights, vs)]

    def heads_full(hs):
        stats, far_o = far_back(hs)
        mixed = mix(hs, keys)
        merged = [merge(h, o[tok:tok + aud, :HD], o[tok:tok + aud, HD:], ma, stats, f)
                  for h, (_, ma, o), f in zip(hs, mixed, far_o)]
        for h, (_, _, o), joined in zip(hs, mixed, merged):
            attn[:, cols(h)] = o[:tok, :HD] / o[:tok, HD:]
            aattn[:, cols(h)] = joined

    def heads_video(hs):
        for h, (mv, ma, o) in zip(hs, mix(hs, span)):
            attn[:, cols(h)] = o[:tok, :HD]
            sums[h] = o[:tok, HD:]
            tops[h] = jnp.broadcast_to(mv, (tok, HD))
            aattn[:, cols(h)] = o[tok:tok + aud, :HD]
            asums[h] = o[tok:tok + aud, HD:]
            atops[h] = jnp.broadcast_to(ma, (aud, HD))

    def heads_audio(hs):
        stats, far_o = far_back(hs)
        loaded = [
            (qown[:, cols(h)], kv[h, 0, pl.ds(span, n * aud)],
             jnp.concatenate([kv[h, 1, pl.ds(span, n * aud)], jnp.ones((n * aud, HD), jnp.bfloat16)], axis=1))
            for h in hs]
        held = [(attn[:, cols(h)], sums[h], tops[h], aattn[:, cols(h)], asums[h], atops[h]) for h in hs]
        scores = [dot_t(q, k) * SCALE for q, k, _ in loaded]
        peaks = [jnp.maximum(jnp.max(s, axis=1, keepdims=True), top) for s, (_, _, top, _, _, _) in zip(scores, held)]
        mixed = [
            jnp.dot(jnp.exp2(s - peak[:, :1]).astype(jnp.bfloat16), v, preferred_element_type=jnp.float32)
            for s, peak, (_, _, v) in zip(scores, peaks, loaded)]
        merged = [merge(h, oa, la, ma, stats, f) for h, (_, _, _, oa, la, ma), f in zip(hs, held, far_o)]
        for h, o, peak, (old, total, top, _, _, _), joined in zip(hs, mixed, peaks, held, merged):
            shrink = jnp.exp2(top - peak)
            attn[:, cols(h)] = (old * shrink + o[:, :HD]) / (total * shrink + o[:, HD:])
            aattn[:, cols(h)] = joined

    def far_sent():
        for slot, exists, device in far:
            @pl.when(exists)
            def _(slot=slot, device=device):
                q_copy(slot, device).wait_send()
                bo_copy(slot, device).wait_send()
                bs_copy(slot, device).wait_send()

    def audio_sent():
        several(chips, s_aud).wait_send()
        for k in range(rows_all):
            count = 1 + (2 + 2 * k) * (k < rows_all - 1) + 2 * (k > 0) + 2 * max(0, k - 1)

            @pl.when(ahead == k)
            def _(count=count):
                several(count, s_link).wait_send()

    pairs = heads // PAIR
    edge = has_src & jnp.logical_not(has_fwd)
    late = has_fwd & (behind >= 2)

    def z_due(i):
        inner = i - LAG_Z + 1 + (edge & (i >= 9)).astype(jnp.int32)
        return jnp.clip(jnp.where(has_src, inner, i + 1), 0, heads)

    def v_due(i):
        inner = jnp.clip((i - LAG_Z) // PAIR, 0, MAIN_PAIRS)
        return jnp.where(has_src, inner, jnp.clip(jnp.where(i < FAR_STEPS, 0, (i - 1) // PAIR), 0, pairs - 1))

    def last_out():
        for p in range(LAST_PIECES):
            y_piece(last, p).start()

    def take_y(h):
        for p in range(pieces(h)):
            with part("ywaitp"):
                y_piece(h, p).wait_recv()

            @pl.when(has_fwd)
            def _(p=p):
                z_piece(h, p).start()

    def take_z(k, _):
        @pl.when(has_src & (k > 0) & (k < last))
        def _():
            with part("zwait"):
                z_copy(k).wait_recv()

        for h in (0, last):
            @pl.when(has_src & (k == h))
            def _(h=h):
                with part("zwaitp"):
                    for p in range(pieces(h)):
                        z_piece(h, p).wait_recv()

        @pl.when((k % PAIR == PAIR - 1) & jnp.logical_not(edge & (k == last)))
        def _():
            d_copy(k // PAIR).start()
        return 0

    def arrive(p):
        with part("dwait"):
            d_copy(p).wait_recv()

    def attend_video(p, _):
        arrive(p)
        with part("vhead"):
            heads_video([p * PAIR + k for k in range(PAIR)])
        return 0

    def attend_audio(g, _):
        with part("ahead"):
            heads_audio([g * CATCH_UP + k for k in range(CATCH_UP)])
        return 0

    def audio_in():
        with part("takeaudio"):
            take_audio()
        with part("layaudio"):
            lax.fori_loop(0, chips, lay_audio, 0)
        with part("bowait"):
            for slot, exists, device in far:
                @pl.when(exists)
                def _(slot=slot):
                    bo_copy(1 - slot, mate).wait_recv()
                    bs_copy(1 - slot, mate).wait_recv()

    def relay(i, _):
        @pl.when((i > 0) & (i < last))
        def _():
            with part("ywait"):
                y_copy(i).wait_recv()

            @pl.when(has_fwd)
            def _():
                z_copy(i).start()

        @pl.when(i + WINDOW < last)
        def _():
            y_copy(i + WINDOW).start()

        @pl.when((i + WINDOW == last) & has_src)
        def _():
            last_out()

        @pl.when(i == 0)
        def _():
            take_y(0)

        @pl.when((i == last) & jnp.logical_not(edge))
        def _():
            take_y(last)

        lax.fori_loop(z_due(i - 1), z_due(i), take_z, 0)

        @pl.when(i == 0)
        def _():
            with part("faropen"):
                far_open()

        @pl.when(i < FAR_STEPS)
        def _():
            with part("far"):
                far_some(i)

        @pl.when(i == FAR_STEPS - 1)
        def _():
            far_close()

        for k, at in enumerate(WAVES[:-1]):
            @pl.when(i == at)
            def _(k=k):
                with part("wave"):
                    wave_step(k)

        @pl.when(i == WAVES[-1])
        def _():
            def more(k, _):
                wave_step(k)
                return 0

            with part("wavelast"):
                lax.fori_loop(len(WAVES) - 1, rows_all, more, 0)

            @pl.when(jnp.logical_not(has_src))
            def _():
                last_out()

        @pl.when(i == BESIDE)
        def _():
            with part("beside"):
                from_behind(1)
                far_sent()

        @pl.when((i == heads - WINDOW) & has_src)
        def _():
            late_across()

        lax.fori_loop(v_due(i - 1), v_due(i), attend_video, 0)
        return 0

    lax.fori_loop(0, heads, relay, 0)

    groups = PAIR * (pairs - 1) // CATCH_UP
    soon = jnp.logical_not(edge | late)
    first_groups = jnp.where(soon, jnp.where(has_src, PAIR * MAIN_PAIRS // CATCH_UP, groups), 0)

    @pl.when(soon)
    def _():
        audio_in()
    lax.fori_loop(0, first_groups, attend_audio, 0)
    lax.fori_loop(z_due(last), heads - 2, take_z, 0)
    lax.fori_loop(v_due(last), pairs - 2, attend_video, 0)
    with part("passaudio"):
        pass_audio()
    lax.fori_loop(jnp.maximum(z_due(last), heads - 2), last, take_z, 0)
    lax.fori_loop(jnp.maximum(v_due(last), pairs - 2), pairs - 1, attend_video, 0)
    lax.fori_loop(jnp.maximum(z_due(last), last), heads, take_z, 0)

    @pl.when(edge)
    def _():
        take_y(last)
        d_copy(pairs - 1).start()

    @pl.when(jnp.logical_not(soon))
    def _():
        audio_in()
    lax.fori_loop(first_groups, groups, attend_audio, 0)
    arrive(pairs - 1)
    with part("head"):
        heads_full([PAIR * (pairs - 1) + k for k in range(PAIR)])

    with part("drain"):
        audio_sent()
        kv_sent = kv.at[:, :, pl.ds(0, 4 * tok)]
        remote(kv_sent, kv_sent, s_kv, r_dk, mate).wait_send()

        @pl.when(has_fwd)
        def _():
            z_sent = kv.at[:, :, pl.ds(0, tok)]
            remote(z_sent, z_sent, s_z, r_dk, mate).wait_send()


def finish_kernel(attn, aattn, vgain, again, vout, aout):
    def finish(mixed, gain):
        scale = lax.rsqrt(jnp.mean(mixed * mixed, axis=1, keepdims=True) + EPS)
        return (mixed * scale * gain[...].reshape(1, mixed.shape[1])).astype(jnp.bfloat16)

    vout[...] = finish(attn[...], vgain)
    aout[...] = finish(aattn[...], again)


def solution(mesh):
    n = mesh.shape["seq"]
    chips = n // 2

    def on_device(vq, vk, vv, aq, ak, av, radius, tile_list, tile_count, vgain, again):
        tok, width = vq.shape
        aud = aq.shape[0]
        heads = width // HD
        keys = 6 * tok + n * aud
        bf, f32 = jnp.bfloat16, jnp.float32
        dma = pltpu.SemaphoreType.DMA
        per_head = dma((heads,))
        hbm = pl.BlockSpec(memory_space=pltpu.HBM)
        vmem = pl.BlockSpec(memory_space=pltpu.VMEM)
        mixed = pl.pallas_call(
            functools.partial(kernel, n, heads, tok, aud, tile_list.shape[1]),
            out_shape=(
                pltpu.VMEM((tok, width), f32), pltpu.VMEM((aud, width), f32),
                pltpu.VMEM((width,), f32), pltpu.VMEM((width,), f32),
            ),
            in_specs=[hbm] * 11,
            out_specs=(vmem,) * 4,
            scratch_shapes=[
                pltpu.SMEM(radius.shape, jnp.int32),
                pltpu.SMEM(tile_list.shape[::-1], jnp.int32),
                pltpu.SMEM(tile_count.shape, jnp.int32),
                pltpu.VMEM((heads, 2, keys, HD), bf),
                pltpu.VMEM((n, 2, aud, width), bf),
                pltpu.VMEM((tok, width), bf),
                pltpu.VMEM((aud, width), bf),
                pltpu.VMEM((2, aud, width), bf),
                pltpu.VMEM((2 * aud, width), bf),
                pltpu.VMEM((2 * aud, width), bf),
                pltpu.VMEM((2, aud, width), bf),
                pltpu.VMEM((2, aud, HD), f32),
                pltpu.VMEM((2, aud, width), bf),
                pltpu.VMEM((2, aud, HD), f32),
                *([pltpu.VMEM((heads, tok, HD), f32)] * 2),
                *([pltpu.VMEM((heads, aud, HD), f32)] * 2),
                dma((8,)), dma((OWN_FIRST + 1,)), dma, dma,
                dma((heads - 2 + FIRST_PIECES + LAST_PIECES,)), dma, dma((heads - 2 + FIRST_PIECES + LAST_PIECES,)), dma((heads // PAIR,)),
                dma, dma((chips,)), dma, dma,
                *([dma((2,))] * 6),
            ],
            compiler_params=pltpu.CompilerParams(
                collective_id=0, has_side_effects=True),
        )(radius, tile_list.T, tile_count, vq, vk, vv, aq, ak, av, vgain, again)
        return pl.pallas_call(
            finish_kernel,
            out_shape=(jax.ShapeDtypeStruct(vq.shape, bf), jax.ShapeDtypeStruct(aq.shape, bf)),
            in_specs=[vmem] * 4,
            out_specs=(vmem, vmem),
            compiler_params=pltpu.CompilerParams(vmem_limit_bytes=8 * 1024 * 1024),
        )(*mixed)

    rows = P(("clips", "seq"), None)
    return jax.shard_map(
        on_device,
        mesh=mesh,
        in_specs=(rows,) * 6 + (P(("clips", "seq")), P("clips", None), P("clips"), P(), P()),
        out_specs=(rows, rows),
        check_vma=False,
    )
```

```python
import contextlib
import functools

import jax
import jax.numpy as jnp
from jax import lax
from jax.experimental import pallas as pl
from jax.experimental.pallas import tpu as pltpu
from jax.sharding import PartitionSpec as P

HD = 128
RMAX = 2
SPAN = 4
LOG2E = 1.4426950408889634
SCALE = HD ** (-0.5) * LOG2E
NEG = -1e30
EPS = 1e-6
MESH = pl.DeviceIdType.MESH
LAG_Z = 4
FAR_STEPS = 4
WAVES = (0, 3, 5, 7)
WAVES_ALONE = (0, 4, 6, 8)
FAR_FIRST = 1
BESIDE = 9
WINDOW = 4
FIRST_PIECES = 2
LAST_PIECES = 4
MAIN_PAIRS = 3
OUT_PIECES = 4
CATCH_UP = 5
PAIR = 2
OWN_FIRST = 2


def part(name):
    return contextlib.nullcontext()


def kernel(
    n, heads, tok, aud, lmax,
    radius_hbm, tile_list_hbm, tile_count_hbm,
    vq_hbm, vk_hbm, vv_hbm, aq_hbm, ak_hbm, av_hbm, vgain_hbm, again_hbm,
    attn, aattn, vgain, again,
    radius, tile_list, tile_count,
    kv, audio, qown, aqown, aqin, qx, qr, part_o, part_s, back_o, back_s, tops, sums, atops, asums,
    load_sem, own_sem, s_kv, r_dk, r_y, s_z, r_z, r_d,
    s_link, r_aud, s_aud, r_daud, s_fo, r_q, r_bo, s_bs, r_bs,
):
    me = lax.axis_index("seq")
    chips = n // 2
    chip = me // 2
    core = me % 2
    mate = chip * 2 + (1 - core)
    odd = chip % 2
    across_chip = chip + 1 - 2 * odd
    across = across_chip * 2 + core
    step = 2 - 4 * odd
    fwd_chip = chip + step
    has_fwd = (fwd_chip >= 0) & (fwd_chip < chips)
    src_chip = chip - step
    has_src = (src_chip >= 0) & (src_chip < chips)
    zchip = chip - 1 + 2 * odd
    fwd = jnp.clip(fwd_chip, 0, chips - 1) * 2 + core

    barrier = pltpu.get_barrier_semaphore()

    def greet(device):
        pl.semaphore_signal(barrier, inc=1, device_id={"seq": device}, device_id_type=MESH)

    low, high = chip >= 2, chip + 2 < chips
    up_to = jnp.clip(chip + 2, 0, chips - 1) * 2 + core
    down_to = jnp.clip(chip - 2, 0, chips - 1) * 2 + core
    greet(across)
    greet(mate)
    for exists, device in ((high, up_to), (low, down_to)):
        @pl.when(exists)
        def _(device=device):
            greet(device)

    loads = [
        pltpu.make_async_copy(aq_hbm, aqown, load_sem.at[0]),
        pltpu.make_async_copy(ak_hbm, audio.at[me, 0], load_sem.at[1]),
        pltpu.make_async_copy(av_hbm, audio.at[me, 1], load_sem.at[1]),
        pltpu.make_async_copy(vq_hbm, qown, load_sem.at[2]),
        pltpu.make_async_copy(vgain_hbm, vgain, load_sem.at[3]),
        pltpu.make_async_copy(again_hbm, again, load_sem.at[4]),
        pltpu.make_async_copy(radius_hbm, radius, load_sem.at[5]),
        pltpu.make_async_copy(tile_list_hbm, tile_list, load_sem.at[6]),
        pltpu.make_async_copy(tile_count_hbm, tile_count, load_sem.at[7]),
    ]

    def cols(h):
        return pl.ds(pl.multiple_of(h * HD, HD), HD)

    def own_head(h):
        return [
            pltpu.make_async_copy(side.at[:, cols(h)], kv.at[h, j, pl.ds(0, tok)], own_sem.at[jnp.minimum(h, OWN_FIRST)])
            for j, side in enumerate((vk_hbm, vv_hbm))
        ]

    for load in loads[:3]:
        load.start()

    def load_own(h, _):
        for load in own_head(h):
            load.start()
        return 0

    lax.fori_loop(0, heads, load_own, 0)
    for load in loads[3:]:
        load.start()

    @pl.when(jnp.logical_not(has_src))
    def _():
        def clear(h, _):
            kv[h, :, pl.ds(3 * tok, tok), :] = jnp.zeros((2, tok, HD), kv.dtype)
            return 0

        lax.fori_loop(0, heads, clear, 0)

    far = [(0, high, up_to), (1, low, down_to)]
    for slot, exists, device in far:
        @pl.when(jnp.logical_not(exists))
        def _(slot=slot):
            aqin[slot] = jnp.zeros(aqin.shape[1:], aqin.dtype)
            back_o[slot] = jnp.zeros(back_o.shape[1:], back_o.dtype)
            back_s[slot] = jnp.zeros(back_s.shape[1:], back_s.dtype)

    with part("barrier"):
        pl.semaphore_wait(barrier, 2 + high.astype(jnp.int32) + low.astype(jnp.int32))

    def remote(src, dst, s, r, device):
        return pltpu.make_async_remote_copy(
            src_ref=src, dst_ref=dst, send_sem=s, recv_sem=r,
            device_id={"seq": device}, device_id_type=MESH)

    def q_copy(slot, device):
        return remote(aqown, aqin.at[1 - slot], s_fo, r_q, device)

    def far_pairs(buffer, sem, fold=1):
        return [
            (exist, remote(buffer.at[pl.ds(0, count * fold)], buffer.at[pl.ds(0, count * fold)], sem, sem, mate))
            for exist, count in ((high & low, 2), (high != low, 1))]

    row, rows_all = chip // 2, chips // 2

    def aud_copy(sem, landed, block, device):
        return remote(audio.at[block], audio.at[block], sem, landed, device)

    def daud_copy(block):
        return aud_copy(s_aud, r_daud, block, mate)

    def link_copy(block, device):
        return aud_copy(s_link, r_aud.at[block // 4], block, device)

    turn = 1 - 2 * odd
    ahead = jnp.where(odd == 1, row, rows_all - 1 - row)
    behind = rows_all - 1 - ahead
    back = jnp.clip(src_chip, 0, chips - 1) * 2 + core

    def at_level(block, k):
        return jnp.clip(block + 4 * k * turn, 0, n - 1)

    def send_on(block):
        @pl.when(has_src)
        def _():
            link_copy(block, back).start()

    def to_front(block):
        @pl.when(has_fwd)
        def _():
            link_copy(block, fwd).start()

    def to_across(first, k):
        @pl.when((k >= 2) & (k <= ahead))
        def _():
            link_copy(at_level(first, k), across).start()

    def wave_step(k):
        @pl.when(k == 0)
        def _():
            several(1, r_aud.at[row]).wait_recv()
            send_on(across)
            to_front(across)
            daud_copy(across).start()

        @pl.when((k > 0) & (k <= ahead))
        def _():
            several(2, r_aud.at[at_level(me, k) // 4]).wait_recv()
            for first in (me, across):
                send_on(at_level(first, k))
                daud_copy(at_level(first, k)).start()

                @pl.when(jnp.logical_not(has_src))
                def _(first=first):
                    to_across(first, k)

    def from_behind(k):
        @pl.when(k <= behind)
        def _():
            several(2, r_aud.at[at_level(me, -k) // 4]).wait_recv()
            for first in (me, across):
                daud_copy(at_level(first, -k)).start()

    def several(count, sem):
        blocks = audio.at[pl.ds(0, count)]
        return remote(blocks, blocks, sem, sem, mate)

    def pass_audio():
        def forward(k, _):
            from_behind(k)
            return 0

        lax.fori_loop(2, rows_all, forward, 0)

    def late_across():
        def send(k, _):
            to_across(me, k)
            to_across(across, k)
            return 0

        lax.fori_loop(2, rows_all, send, 0)

    def take_audio():
        several(chips, r_daud).wait_recv()

    def kv_head(slot, h):
        return kv.at[h, :, pl.ds(slot * tok, tok)]

    last = heads - 1

    def y_copy(h):
        return remote(kv_head(0, h), kv_head(2, h), s_kv, r_y.at[FIRST_PIECES + h - 1], across)

    def z_copy(h):
        return remote(kv_head(2, h), kv_head(3, h), s_z, r_z.at[h // PAIR], fwd)

    def pieces(h):
        return FIRST_PIECES if h == 0 else LAST_PIECES

    def piece(slot, h, p):
        count = tok // pieces(h)
        return kv.at[h, :, pl.ds(slot * tok + p * count, count)]

    def piece_sem(h, p):
        return (0 if h == 0 else FIRST_PIECES + heads - 2) + p

    def y_piece(h, p):
        return remote(piece(0, h, p), piece(2, h, p), s_kv, r_y.at[piece_sem(h, p)], across)

    def z_piece(h, p):
        return remote(piece(2, h, p), piece(3, h, p), s_z, r_z.at[0 if h == 0 else heads // PAIR], fwd)

    def d_copy(p):
        heads_of = pl.ds(PAIR * p, PAIR)
        return remote(
            kv.at[heads_of, :, pl.ds(2 * tok, 2 * tok)], kv.at[heads_of, :, pl.ds(4 * tok, 2 * tok)], s_kv, r_d.at[p], mate)

    def d_last(share):
        if share == 0:
            there = [kv.at[pl.ds(last - 1, PAIR), :, pl.ds(slot * tok, tok)] for slot in (2, 4)]
        else:
            there = [kv.at[last - PAIR + share, :, pl.ds(slot * tok, tok)] for slot in (3, 5)]
        return remote(*there, s_kv, r_d.at[last // PAIR], mate)

    dk = remote(kv.at[:, :, pl.ds(0, tok)], kv.at[:, :, pl.ds(tok, tok)], s_kv, r_dk, mate)

    def own_there(first, count):
        there = kv.at[pl.ds(first, count), :, pl.ds(0, tok)]
        pltpu.make_async_copy(there, there, own_sem.at[min(first, OWN_FIRST)]).wait()

    own_there(0, 1)
    for p in range(FIRST_PIECES):
        y_piece(0, p).start()
    pltpu.make_async_copy(audio.at[me], audio.at[me], load_sem.at[1]).wait()
    link_copy(me, across).start()
    for h in range(1, OWN_FIRST):
        own_there(h, 1)
        y_copy(h).start()
    loads[0].wait()
    for slot, exists, device in far:
        @pl.when(exists)
        def _(slot=slot, device=device):
            q_copy(slot, device).start()

    send_on(me)
    to_front(me)
    own_there(OWN_FIRST, heads - OWN_FIRST)
    for h in range(OWN_FIRST, WINDOW):
        y_copy(h).start()
    daud_copy(me).start()
    dk.start()

    for load in loads[3:9]:
        load.wait()
    wide = jnp.concatenate([aqown[...].astype(jnp.float32), jnp.zeros((aud, heads * HD), jnp.float32)], axis=0)
    qx[...] = wide.astype(jnp.bfloat16)

    def dot_t(a, b):
        return lax.dot_general(a, b, (((1,), (1,)), ((), ())), preferred_element_type=jnp.float32)

    def is_listed(block, tile):
        listed = jnp.int32(0)
        for j in range(lmax):
            listed = jnp.where((tile_list[j, block] == tile) & (j < tile_count[block]), 1, listed)
        return listed > 0

    def bias_of(seen):
        return jnp.where(seen, 0.0, NEG).astype(jnp.float32)

    tiles = [me, mate, across, zchip * 2 + core, across_chip * 2 + 1 - core, zchip * 2 + 1 - core]
    near = radius[0]
    see_v, see_a = [], []
    for tile in tiles:
        inside = (tile >= 0) & (tile < n)
        see_v.append(bias_of(inside & (jnp.abs(tile - me) <= near)))
        see_a.append(bias_of(inside & is_listed(me, tile)))
    upper = lax.broadcasted_iota(jnp.int32, (2 * aud, tok), 0) < aud
    see_far = [
        jnp.where(upper, bias_of(is_listed(up_to, tile)), bias_of(is_listed(down_to, tile)))
        for tile in (me, mate)
    ]
    far_there = [bias_of(exists) for _, exists, _ in far]

    lane = lax.broadcasted_iota(jnp.int32, (aud, HD), 1)

    def far_group(hs):
        loaded = [(qr[:, cols(h)], kv[h, 0, pl.ds(0, 2 * tok)], kv[h, 1, pl.ds(0, 2 * tok)]) for h in hs]
        scores = [dot_t(q, k) for q, k, _ in loaded]
        results = []
        for s, (_, _, v) in zip(scores, loaded):
            sides = [s[:, j * tok:(j + 1) * tok] * SCALE + see_far[j] for j in range(2)]
            m = jnp.max(jnp.maximum(*sides), axis=1, keepdims=True)
            w = jnp.concatenate([jnp.exp2(side - m).astype(jnp.bfloat16) for side in sides], axis=1)
            ones = jnp.ones((2 * tok, HD), jnp.bfloat16)
            results.append((m, jnp.dot(w, jnp.concatenate([v, ones], axis=1), preferred_element_type=jnp.float32)))
        stats = [part_s[slot] for slot in range(2)]
        for h, (m, o) in zip(hs, results):
            mean = (o[:, :HD] / o[:, HD:]).astype(part_o.dtype).astype(jnp.float32)
            for slot in range(2):
                rows = slice(slot * aud, (slot + 1) * aud)
                part_o[slot, :, cols(h)] = mean[rows].astype(part_o.dtype)
                stats[slot] = jnp.where(lane == h, m[rows], stats[slot])
                stats[slot] = jnp.where(lane == h + 64, o[rows, HD:], stats[slot])
        for slot in range(2):
            part_s[slot] = stats[slot]

    def bo_copy(slot, device):
        return remote(part_o.at[slot], back_o.at[1 - slot], s_fo, r_bo, device)

    def bs_copy(slot, device):
        return remote(part_s.at[slot], back_s.at[1 - slot], s_bs, r_bs, device)

    def far_open():
        dk.wait_recv()
        for exist, copy in far_pairs(aqin, r_q):
            pl.when(exist)(copy.wait_recv)
        both = jnp.concatenate([aqin[0].astype(jnp.float32), aqin[1].astype(jnp.float32)], axis=0)
        qr[...] = both.astype(jnp.bfloat16)
        part_s[...] = jnp.zeros(part_s.shape, jnp.float32)

    far_each = -(-heads // FAR_STEPS)

    def far_some(i):
        far_group([jnp.minimum(i * far_each + j, heads - 1) for j in range(far_each)])

    def far_close():
        for slot, exists, device in far:
            @pl.when(exists)
            def _(slot=slot, device=device):
                bo_copy(slot, device).start()
                bs_copy(slot, device).start()

    def lay_audio(i, _):
        for j in range(2):
            pair = jnp.concatenate(
                [audio[2 * i, j].astype(jnp.float32), audio[2 * i + 1, j].astype(jnp.float32)], axis=0)
            pair = pair.astype(jnp.bfloat16)
            for h in range(heads):
                kv[h, j, pl.ds(pl.multiple_of(6 * tok + 2 * aud * i, 2 * aud), 2 * aud), :] = pair[:, h * HD:(h + 1) * HD]
        return 0

    span = 6 * tok
    keys = span + n * aud

    def row_sum(parts):
        wide = [p.astype(jnp.float32) for p in parts]
        same = [p for p in wide if p.shape == wide[0].shape]
        rest = [p for p in wide if p.shape != wide[0].shape]
        total = jnp.sum(functools.reduce(jnp.add, same), axis=1, keepdims=True)
        return functools.reduce(jnp.add, [jnp.sum(p, axis=1, keepdims=True) for p in rest], total)

    def softmax_part(s, biases):
        blocks = [s[:, i * tok:(i + 1) * tok] * SCALE + biases[i] for i in range(len(biases))]
        if s.shape[1] > len(biases) * tok:
            blocks.append(s[:, len(biases) * tok:] * SCALE)
        m = functools.reduce(jnp.maximum, [jnp.max(b, axis=1, keepdims=True) for b in blocks]) if blocks[-1].shape[1] != tok else jnp.max(functools.reduce(jnp.maximum, blocks), axis=1, keepdims=True)
        parts = [jnp.exp2(b - m).astype(jnp.bfloat16) for b in blocks]
        return m, row_sum(parts), jnp.concatenate(parts, axis=1)

    def merge(h, oa, la, ma, stats, far_o):
        peaks, totals = [], []
        for slot in range(2):
            st = stats[slot]
            peaks.append(jnp.max(jnp.where(lane == h, st, NEG), axis=1, keepdims=True) + far_there[slot])
            totals.append(jnp.sum(jnp.where(lane == h + 64, st, 0.0), axis=1, keepdims=True))
        peak = functools.reduce(jnp.maximum, peaks, ma)
        shrink = jnp.exp2(ma - peak)
        oa = oa * shrink
        la = la * shrink
        for slot in range(2):
            share = jnp.exp2(peaks[slot] - peak) * totals[slot]
            oa = oa + far_o[slot].astype(jnp.float32) * share
            la = la + share
        return oa / la

    def far_back(hs):
        return [back_s[slot] for slot in range(2)], [[back_o[slot, :, cols(h)] for slot in range(2)] for h in hs]

    def mix(hs, width):
        qs = [jnp.concatenate([qown[:, cols(h)], qx[:, cols(h)]], axis=0) for h in hs]
        ks = [kv[h, 0, pl.ds(0, width)] for h in hs]
        vs = [kv[h, 1, pl.ds(0, width)] for h in hs]
        scores = [dot_t(q, k) for q, k in zip(qs, ks)]
        weights = []
        for s in scores:
            mv, lv, wv = softmax_part(s[:tok], see_v)
            ma, la, wa = softmax_part(s[tok:, :span], see_a)
            if width > span:
                wa = jnp.concatenate([wa, jnp.zeros((2 * aud, width - span), jnp.bfloat16)], axis=1)
            weights.append((mv, lv, ma[:aud], la[:aud], jnp.concatenate([wv, wa], axis=0)))
        return [(mv, lv, ma, la, jnp.dot(w, v, preferred_element_type=jnp.float32))
                for (mv, lv, ma, la, w), v in zip(weights, vs)]

    def heads_full(hs):
        stats, far_o = far_back(hs)
        mixed = mix(hs, keys)
        merged = [merge(h, o[tok:tok + aud], la, ma, stats, f)
                  for h, (_, _, ma, la, o), f in zip(hs, mixed, far_o)]
        for h, (_, lv, _, _, o), joined in zip(hs, mixed, merged):
            attn[:, cols(h)] = o[:tok] / lv
            aattn[:, cols(h)] = joined

    def heads_video(hs):
        for h, (mv, lv, ma, la, o) in zip(hs, mix(hs, span)):
            attn[:, cols(h)] = o[:tok]
            sums[h] = jnp.broadcast_to(lv, (tok, HD))
            tops[h] = jnp.broadcast_to(mv, (tok, HD))
            aattn[:, cols(h)] = o[tok:tok + aud]
            asums[h] = jnp.broadcast_to(la, (aud, HD))
            atops[h] = jnp.broadcast_to(ma, (aud, HD))

    def row_peak(peak, s):
        return peak if peak.shape == s.shape else peak[:, :1]

    def heads_audio(hs):
        stats, far_o = far_back(hs)
        loaded = [
            (qown[:, cols(h)], kv[h, 0, pl.ds(span, n * aud)],
             jnp.concatenate([kv[h, 1, pl.ds(span, n * aud)], jnp.ones((n * aud, HD), jnp.bfloat16)], axis=1))
            for h in hs]
        held = [(attn[:, cols(h)], sums[h], tops[h], aattn[:, cols(h)], asums[h], atops[h]) for h in hs]
        scores = [dot_t(q, k) * SCALE for q, k, _ in loaded]
        peaks = [jnp.maximum(jnp.max(s, axis=1, keepdims=True), top) for s, (_, _, top, _, _, _) in zip(scores, held)]
        mixed = [
            jnp.dot(jnp.exp2(s - row_peak(peak, s)).astype(jnp.bfloat16), v, preferred_element_type=jnp.float32)
            for s, peak, (_, _, v) in zip(scores, peaks, loaded)]
        merged = [merge(h, oa, la, ma, stats, f) for h, (_, _, _, oa, la, ma), f in zip(hs, held, far_o)]
        for h, o, peak, (old, total, top, _, _, _), joined in zip(hs, mixed, peaks, held, merged):
            shrink = jnp.exp2(top - peak)
            attn[:, cols(h)] = (old * shrink + o[:, :HD]) / (total * shrink + o[:, HD:])
            aattn[:, cols(h)] = joined

    def far_sent():
        for exist, copy in far_pairs(part_o, s_fo, 2) + far_pairs(part_s, s_bs):
            pl.when(exist)(copy.wait_send)

    def audio_sent():
        several(chips, s_aud).wait_send()
        for k in range(rows_all):
            count = 1 + (2 + 2 * k) * (k < rows_all - 1) + 2 * (k > 0) + 2 * max(0, k - 1)

            @pl.when(ahead == k)
            def _(count=count):
                several(count, s_link).wait_send()

    pairs = heads // PAIR
    edge = has_src & jnp.logical_not(has_fwd)
    late = has_fwd & (behind >= 2)

    def z_due(i):
        inner = (i - LAG_Z + 1 + (edge & (i == last - 1)).astype(jnp.int32)) // PAIR
        return jnp.clip(jnp.where(has_src, inner, (i + 1) // PAIR), 0, pairs - 1)

    def v_due(i):
        inner = jnp.clip((i - LAG_Z) // PAIR, 0, MAIN_PAIRS)
        return jnp.where(has_src, inner, jnp.clip(jnp.where(i < FAR_STEPS + FAR_FIRST, 0, (i - 1) // PAIR), 0, pairs - 1))

    def last_out():
        for p in range(LAST_PIECES):
            y_piece(last, p).start()

    def take_y(h):
        for p in range(pieces(h)):
            with part("ywaitp"):
                y_piece(h, p).wait_recv()

            @pl.when(has_fwd)
            def _(p=p):
                z_piece(h, p).start()

    def z_there(first, count, sem):
        @pl.when(has_src)
        def _():
            with part("zwait"):
                there = kv.at[pl.ds(first, count), :, pl.ds(3 * tok, tok)]
                remote(there, there, s_z, r_z.at[sem], fwd).wait_recv()

    def take_z(p, _):
        z_there(PAIR * p, PAIR, p)
        d_copy(p).start()
        return 0

    def take_last(share):
        z_there(last - PAIR + share, 1, pairs - 2 + share)
        d_last(share).start()

    def arrive(p):
        with part("dwait"):
            d_copy(p).wait_recv()

    def attend_video(p, _):
        arrive(p)
        with part("vhead"):
            heads_video([p * PAIR + k for k in range(PAIR)])
        return 0

    def attend_audio(g, _):
        with part("ahead"):
            heads_audio([g * CATCH_UP + k for k in range(CATCH_UP)])
        return 0

    def audio_in():
        with part("takeaudio"):
            take_audio()
        with part("layaudio"):
            lax.fori_loop(0, chips, lay_audio, 0)
        with part("bowait"):
            for exist, copy in far_pairs(back_o, r_bo) + far_pairs(back_s, r_bs):
                pl.when(exist)(copy.wait_recv)

    def relay(i, _):
        @pl.when((i > 0) & (i < last))
        def _():
            with part("ywait"):
                y_copy(i).wait_recv()

            @pl.when(has_fwd)
            def _():
                z_copy(i).start()

        @pl.when(i + WINDOW < last)
        def _():
            y_copy(i + WINDOW).start()

        @pl.when((i + WINDOW == last) & has_src)
        def _():
            last_out()

        @pl.when(i == 0)
        def _():
            take_y(0)

        @pl.when((i == last) & jnp.logical_not(edge))
        def _():
            take_y(last)
            d_last(0).start()

        lax.fori_loop(z_due(i - 1), z_due(i), take_z, 0)

        @pl.when(i == FAR_FIRST)
        def _():
            with part("faropen"):
                far_open()

        @pl.when((i >= FAR_FIRST) & (i < FAR_FIRST + FAR_STEPS))
        def _():
            with part("far"):
                far_some(i - FAR_FIRST)

        @pl.when(i == FAR_FIRST + FAR_STEPS - 1)
        def _():
            far_close()

        for k, at in enumerate(zip(WAVES[:-1], WAVES_ALONE[:-1])):
            @pl.when(i == jnp.where(has_src, *at))
            def _(k=k):
                with part("wave"):
                    wave_step(k)

        @pl.when(i == jnp.where(has_src, WAVES[-1], WAVES_ALONE[-1]))
        def _():
            def more(k, _):
                wave_step(k)
                return 0

            with part("wavelast"):
                lax.fori_loop(len(WAVES) - 1, rows_all, more, 0)

            @pl.when(jnp.logical_not(has_src))
            def _():
                last_out()

        @pl.when(i == BESIDE)
        def _():
            with part("beside"):
                from_behind(1)
                far_sent()

        @pl.when((i == heads - WINDOW) & has_src)
        def _():
            late_across()

        lax.fori_loop(v_due(i - 1), v_due(i), attend_video, 0)
        return 0

    lax.fori_loop(0, heads, relay, 0)

    groups = PAIR * (pairs - 1) // CATCH_UP
    soon = jnp.logical_not(edge | late)
    first_groups = jnp.where(soon, jnp.where(has_src, PAIR * MAIN_PAIRS // CATCH_UP, groups), 0)

    @pl.when(soon)
    def _():
        audio_in()
    lax.fori_loop(0, first_groups, attend_audio, 0)
    lax.fori_loop(z_due(last), pairs - 1, take_z, 0)
    @pl.when(edge)
    def _():
        with part("passaudio"):
            pass_audio()
    lax.fori_loop(v_due(last), pairs - 2, attend_video, 0)

    @pl.when(late)
    def _():
        with part("passaudio"):
            pass_audio()
    lax.fori_loop(jnp.maximum(v_due(last), pairs - 2), pairs - 1, attend_video, 0)
    take_last(1)
    take_last(2)

    @pl.when(edge)
    def _():
        take_y(last)
        d_last(0).start()

    @pl.when(jnp.logical_not(soon))
    def _():
        audio_in()
    lax.fori_loop(first_groups, groups, attend_audio, 0)
    with part("dwait"):
        d_copy(pairs - 1).wait_recv()
    with part("head"):
        heads_full([PAIR * (pairs - 1) + k for k in range(PAIR)])

    with part("drain"):
        audio_sent()
        kv_sent = kv.at[:, :, pl.ds(0, 4 * tok)]
        remote(kv_sent, kv_sent, s_kv, r_dk, mate).wait_send()

        @pl.when(has_fwd)
        def _():
            z_sent = kv.at[:, :, pl.ds(0, tok)]
            remote(z_sent, z_sent, s_z, r_dk, mate).wait_send()


def finish_kernel(attn, aattn, vgain, again, vout, aout, vbuf, abuf, sems):
    def finish(mixed, gain):
        scale = lax.rsqrt(jnp.mean(mixed * mixed, axis=1, keepdims=True) + EPS)
        return (mixed * scale * gain[...].reshape(1, mixed.shape[1])).astype(jnp.bfloat16)

    rows = vbuf.shape[0] // OUT_PIECES
    copies = []
    for p in range(OUT_PIECES):
        at = pl.ds(p * rows, rows)
        vbuf[at, :] = finish(attn[at, :], vgain)
        copies.append(pltpu.make_async_copy(vbuf.at[at], vout.at[at], sems.at[p]))
        copies[-1].start()
    abuf[...] = finish(aattn[...], again)
    copies.append(pltpu.make_async_copy(abuf, aout, sems.at[OUT_PIECES]))
    copies[-1].start()
    for copy in copies:
        copy.wait()


def solution(mesh):
    n = mesh.shape["seq"]
    chips = n // 2

    def on_device(vq, vk, vv, aq, ak, av, radius, tile_list, tile_count, vgain, again):
        tok, width = vq.shape
        aud = aq.shape[0]
        heads = width // HD
        keys = 6 * tok + n * aud
        bf, f32 = jnp.bfloat16, jnp.float32
        dma = pltpu.SemaphoreType.DMA
        per_head = dma((heads,))
        hbm = pl.BlockSpec(memory_space=pltpu.HBM)
        vmem = pl.BlockSpec(memory_space=pltpu.VMEM)
        mixed = pl.pallas_call(
            functools.partial(kernel, n, heads, tok, aud, tile_list.shape[1]),
            out_shape=(
                pltpu.VMEM((tok, width), f32), pltpu.VMEM((aud, width), f32),
                pltpu.VMEM((width,), f32), pltpu.VMEM((width,), f32),
            ),
            in_specs=[hbm] * 11,
            out_specs=(vmem,) * 4,
            scratch_shapes=[
                pltpu.SMEM(radius.shape, jnp.int32),
                pltpu.SMEM(tile_list.shape[::-1], jnp.int32),
                pltpu.SMEM(tile_count.shape, jnp.int32),
                pltpu.VMEM((heads, 2, keys, HD), bf),
                pltpu.VMEM((n, 2, aud, width), bf),
                pltpu.VMEM((tok, width), bf),
                pltpu.VMEM((aud, width), bf),
                pltpu.VMEM((2, aud, width), bf),
                pltpu.VMEM((2 * aud, width), bf),
                pltpu.VMEM((2 * aud, width), bf),
                pltpu.VMEM((4, aud, width), bf),
                pltpu.VMEM((2, aud, HD), f32),
                pltpu.VMEM((2, aud, width), bf),
                pltpu.VMEM((2, aud, HD), f32),
                *([pltpu.VMEM((heads, tok, HD), f32)] * 2),
                *([pltpu.VMEM((heads, aud, HD), f32)] * 2),
                dma((8,)), dma((OWN_FIRST + 1,)), dma, dma,
                dma((heads - 2 + FIRST_PIECES + LAST_PIECES,)), dma, dma((heads // PAIR + 1,)), dma((heads // PAIR,)),
                dma, dma((chips // 2,)), dma, dma,
                *([dma] * 5),
            ],
            compiler_params=pltpu.CompilerParams(
                collective_id=0, has_side_effects=True),
        )(radius, tile_list.T, tile_count, vq, vk, vv, aq, ak, av, vgain, again)
        return pl.pallas_call(
            finish_kernel,
            out_shape=(jax.ShapeDtypeStruct(vq.shape, bf), jax.ShapeDtypeStruct(aq.shape, bf)),
            in_specs=[vmem] * 4,
            out_specs=(hbm, hbm),
            scratch_shapes=[pltpu.VMEM(vq.shape, bf), pltpu.VMEM(aq.shape, bf), dma((OUT_PIECES + 1,))],
            compiler_params=pltpu.CompilerParams(vmem_limit_bytes=8 * 1024 * 1024),
        )(*mixed)

    rows = P(("clips", "seq"), None)
    return jax.shard_map(
        on_device,
        mesh=mesh,
        in_specs=(rows,) * 6 + (P(("clips", "seq")), P("clips", None), P("clips"), P(), P()),
        out_specs=(rows, rows),
        check_vma=False,
    )
```
